32 devices in a mesh: outer: 4 (over y, core), inner: 8 (over z, x).
Axes of the slice: x: 2, y: 2, z: 4, core: 2. Of those that a mesh axis runs over, the one named last changes fastest.
Arguments:
- tokens: bfloat16 [12288, 4096], P(('outer', 'inner')), may hold values from -6 to 6
- out_grad: bfloat16 [12288, 1024], P(('outer', 'inner')), may hold values from -0.3125 to 0.3125
- master_weights: float32 [1024, 4096], P(('outer', 'inner')), may hold values from -0.0421 to 0.0421
- base_weights: bfloat16 [1024, 4096], replicated, may hold values from -0.030029297 to 0.030029297
- adam_m: float32 [1024, 4096], P(('outer', 'inner')), may hold values from -8 to 8
- adam_v: float32 [1024, 4096], P(('outer', 'inner')), may hold values from 0.1 to 10
- grad_exps: int32 [32, 8, 32], P(('outer', 'inner')), may hold values from -13 to -8
- diff_exps: int32 [1024, 32], P(('outer', 'inner')), may hold values from -20 to -15
- hadamard_signs: int32 [32, 128], replicated, may hold values 0 or 1
Outputs:
- projected: bfloat16 [12288, 1024], P(('outer', 'inner'))
- new_master: float32 [1024, 4096], P(('outer', 'inner'))
- new_first: float32 [1024, 4096], P(('outer', 'inner'))
- new_second: float32 [1024, 4096], P(('outer', 'inner'))
The draws below stay inside these ranges and needn't reach their ends.
All inputs are finite; a program needn't handle non-finite values.
Results may differ from the reference program's by a relative error of at most 0.005.
Values may be sent and summed in bfloat16 or wider, within the bound.
A program may use at most 128 MiB of HBM per device.

```python
import math
import jax
import jax.numpy as jnp
from jax import lax

D = 4096
KV = 1024
HB = 128
ADAM_STEP = 10
TOK_DEV = 384
BLOCKS = 32
TOKENS = 12288


def shared_weights(key):
    base_key = jax.random.fold_in(key, 11)
    drift_key = jax.random.fold_in(key, 23)
    base_rows = jax.random.uniform(base_key, (KV, D), jnp.float32, -0.03, 0.03)
    drift_rows = jax.random.truncated_normal(drift_key, -4.0, 4.0, (KV, D), jnp.float32) * 0.003
    base_half = base_rows.astype(jnp.bfloat16)
    return (base_half, base_half.astype(jnp.float32) + drift_rows)


def draw_base_weights(key, part):
    return shared_weights(key)[0]


def draw_master_weights(key, part):
    return shared_weights(key)[1]


def with_ends(array, own_key, smallest, top_value):
    longest = array.shape.index(max(array.shape))
    spots = []
    for shift in (0, 1):
        where = [jax.random.randint(jax.random.fold_in(own_key, axis), (), 0, length) for axis, length in enumerate(array.shape)]
        where[longest] = (where[longest] + shift) % array.shape[longest]
        spots.append(tuple(where))
    return array.at[spots[0]].set(smallest).at[spots[1]].set(top_value)


def raised(result, key, source, target, shards_of, factor):
    def block_of(dim):
        return (jnp.arange(result.shape[dim]) // (result.shape[dim] // shards_of)).reshape((-1,) + (1,) * (result.ndim - 1 - dim))

    one_side = jax.random.permutation(key, shards_of)[block_of(target)]
    far = (block_of(target) + shards_of // 2) % shards_of
    return jnp.where((block_of(source) == one_side) | (block_of(source) == far), factor * result, result)


def levels(own_key, dims, cuts, smallest, high):
    level = 1.0
    for axis_at, blocks in cuts:
        draws = jax.random.uniform(jax.random.fold_in(jax.random.fold_in(own_key, 6), axis_at), (blocks,), jnp.float32, smallest / len(cuts), high / len(cuts))
        level = level * jnp.repeat(jnp.exp(draws), dims[axis_at] // blocks).reshape((-1,) + (1,) * (len(dims) - 1 - axis_at))
    return level


def gaussian(stream_key, shape, scale, reach, shards=(), held_as=jnp.bfloat16):
    factor_of = levels(stream_key, shape, shards, -0.22, 0.18) if shards else 1.0
    drawn = jax.random.normal(stream_key, shape, jnp.float32) * scale * factor_of
    return jnp.minimum(jnp.maximum(drawn, -reach), reach).astype(held_as)


def gaussian_with(own_key, dims, spread, limit, cuts, heavy, kind=jnp.bfloat16):
    array = spread * jax.random.normal(own_key, dims, jnp.float32)
    if cuts:
        array = array * levels(own_key, dims, cuts, -0.22, 0.18)
    return jnp.clip(raised(array, jax.random.fold_in(own_key, 3), *heavy), -limit, limit).astype(kind)


def setup_inputs(seed: int = 0) -> dict:
    seeds = jax.random.split(jax.random.key(seed), 10)
    tokens = gaussian(seeds[0], (TOKENS, D), 1.0, 6.0, ((0, 32),))
    out_grad = gaussian_with(seeds[1], (TOKENS, KV), (TOKENS // 9) ** -0.5, 0.3125, ((0, 32),), (0, 1, 32, 2.75))
    master_weights = draw_master_weights(jax.random.fold_in(seeds[9], 71), 0)
    base_weights = draw_base_weights(jax.random.fold_in(seeds[9], 71), 0)
    adam_m = gaussian(seeds[4], (KV, D), 2.0, 8.0, ((0, 32),), jnp.float32)
    adam_v = jnp.clip(jnp.exp(math.log(10.0) - 4.6051702 * jax.random.uniform(seeds[5], (KV, D), jnp.float32) ** levels(seeds[5], (KV, D), ((0, 32),), -0.2, 0.2)), 0.1, 10.0)
    grad_exps = with_ends(jax.random.randint(seeds[6], (BLOCKS, KV // HB, D // HB), -13, -7), jax.random.fold_in(seeds[6], 1), -13, (-7) - 1).astype(jnp.int32)
    diff_exps = with_ends(jax.random.randint(seeds[7], (KV, D // HB), -20, -14), jax.random.fold_in(seeds[7], 1), -20, (-14) - 1).astype(jnp.int32)
    hadamard_signs = with_ends((jax.random.randint(seeds[8], (D // HB, HB), 0, 2) < 1).astype(jnp.int32), jax.random.fold_in(seeds[8], 1), 0, 1)
    return {"tokens": tokens, "out_grad": out_grad, "master_weights": master_weights, "base_weights": base_weights, "adam_m": adam_m, "adam_v": adam_v, "grad_exps": grad_exps, "diff_exps": diff_exps, "hadamard_signs": hadamard_signs}


clip_level = 448.0
beta_one = 0.9
beta_two = 0.95
learn_rate = 0.002
decay_rate = 0.1
adam_eps = 1e-08
highest = lax.Precision.HIGHEST

def hadamard(matrix_size):
    positions = jnp.arange(matrix_size, dtype=jnp.int32)
    common = positions[:, None] & positions[None, :]
    parity = jnp.zeros((matrix_size, matrix_size), jnp.int32)
    for bit_level in range(matrix_size.bit_length() - 1):
        parity = parity + (common >> bit_level & 1)
    return (1 - 2 * (parity % 2)).astype(jnp.float32)

def rotate_rows(row_block, sign_rows, matrix):
    row_count = row_block.shape[0]
    blocks = row_block.reshape(row_count, sign_rows.shape[0], sign_rows.shape[1]) * sign_rows
    turned = jnp.dot(blocks.reshape(-1, sign_rows.shape[1]), matrix, precision=highest)
    return turned.reshape(row_block.shape) / math.sqrt(sign_rows.shape[1])

def unrotate_rows(row_block, sign_rows, matrix):
    row_count = row_block.shape[0]
    turned = jnp.dot(row_block.reshape(-1, sign_rows.shape[1]), matrix, precision=highest) / math.sqrt(sign_rows.shape[1])
    return (turned.reshape(row_count, sign_rows.shape[0], sign_rows.shape[1]) * sign_rows).reshape(row_block.shape)

def clip_rows(row_block, bound_rows):
    row_count = row_block.shape[0]
    shaped = row_block.reshape(row_count, bound_rows.shape[1], -1)
    limits = bound_rows[:, :, None]
    return jnp.clip(shaped, -limits, limits).reshape(row_block.shape)

def adam_update(gradient, master, first, second):
    new_first = beta_one * first + (1.0 - beta_one) * gradient
    new_second = beta_two * second + (1.0 - beta_two) * gradient * gradient
    fix_one = 1.0 - beta_one ** ADAM_STEP
    fix_two = 1.0 - beta_two ** ADAM_STEP
    step_dir = new_first / fix_one / (jnp.sqrt(new_second / fix_two) + adam_eps)
    new_master = master - learn_rate * (step_dir + decay_rate * master)
    return (new_master, new_first, new_second)

def reference(tokens, out_grad, master_weights, base_weights, adam_m, adam_v, grad_exps, diff_exps, hadamard_signs):
    sign_rows = (2 * hadamard_signs - 1).astype(jnp.float32)
    matrix = hadamard(HB)

    def add_block(total, block_id):
        rows_x = lax.dynamic_slice_in_dim(tokens, block_id * TOK_DEV, TOK_DEV, 0)
        rows_g = lax.dynamic_slice_in_dim(out_grad, block_id * TOK_DEV, TOK_DEV, 0)
        term_rows = lax.dot_general(rows_g, rows_x, (((0,), (0,)), ((), ())), preferred_element_type=jnp.float32)
        turned = rotate_rows(term_rows, sign_rows, matrix)
        exps_here = lax.dynamic_index_in_dim(grad_exps, block_id, 0, keepdims=False)
        bound_rows = jnp.repeat(clip_level * jnp.exp2(exps_here.astype(jnp.float32)), HB, axis=0)
        coded_rows = lax.optimization_barrier(clip_rows(turned, bound_rows).astype(jnp.bfloat16))
        return (total + coded_rows.astype(jnp.float32), None)
    summed, unused = lax.scan(add_block, jnp.zeros((KV, D), jnp.float32), jnp.arange(BLOCKS, dtype=jnp.int32))
    gradient = unrotate_rows(summed, sign_rows, matrix)
    new_master, new_first, new_second = adam_update(gradient, master_weights, adam_m, adam_v)
    base_full = base_weights.astype(jnp.float32)
    diff_bound = clip_level * jnp.exp2(diff_exps.astype(jnp.float32))
    diff_coded = lax.optimization_barrier(clip_rows(new_master - base_full, diff_bound).astype(jnp.bfloat16))
    effective = (base_full + diff_coded.astype(jnp.float32)).astype(jnp.bfloat16)
    projected = lax.dot_general(tokens, effective, (((1,), (1,)), ((), ())), preferred_element_type=jnp.float32)
    return (projected.astype(jnp.bfloat16), new_master, new_first, new_second)
```

```python
import functools
import math

import jax
import jax.numpy as jnp
from jax import lax
from jax.experimental import pallas as pl
from jax.experimental.pallas import tpu as pltpu
from jax.sharding import PartitionSpec as P

ADAM_STEP = 10


clip_level = 448.0
beta_one = 0.9
beta_two = 0.95
learn_rate = 0.002
decay_rate = 0.1
adam_eps = 1e-08
highest = lax.Precision.HIGHEST


def hadamard(matrix_size):
    positions = jnp.arange(matrix_size, dtype=jnp.int32)
    common = positions[:, None] & positions[None, :]
    parity = jnp.zeros((matrix_size, matrix_size), jnp.int32)
    for bit_level in range(matrix_size.bit_length() - 1):
        parity = parity + (common >> bit_level & 1)
    return (1 - 2 * (parity % 2)).astype(jnp.float32)


def rotate_rows(row_block, sign_rows, matrix):
    row_count = row_block.shape[0]
    blocks = row_block.reshape(row_count, sign_rows.shape[0], sign_rows.shape[1]) * sign_rows
    turned = jnp.dot(blocks.reshape(-1, sign_rows.shape[1]), matrix, precision=highest)
    return turned.reshape(row_block.shape) / math.sqrt(sign_rows.shape[1])


def unrotate_rows(row_block, sign_rows, matrix):
    row_count = row_block.shape[0]
    turned = jnp.dot(
        row_block.reshape(-1, sign_rows.shape[1]), matrix, precision=highest
    ) / math.sqrt(sign_rows.shape[1])
    return (turned.reshape(row_count, sign_rows.shape[0], sign_rows.shape[1]) * sign_rows).reshape(
        row_block.shape
    )


def clip_rows(row_block, bound_rows):
    row_count = row_block.shape[0]
    shaped = row_block.reshape(row_count, bound_rows.shape[1], -1)
    limits = bound_rows[:, :, None]
    return jnp.clip(shaped, -limits, limits).reshape(row_block.shape)


def adam_update(gradient, master, first, second):
    new_first = beta_one * first + (1.0 - beta_one) * gradient
    new_second = beta_two * second + (1.0 - beta_two) * gradient * gradient
    fix_one = 1.0 - beta_one**ADAM_STEP
    fix_two = 1.0 - beta_two**ADAM_STEP
    step_dir = new_first / fix_one / (jnp.sqrt(new_second / fix_two) + adam_eps)
    new_master = master - learn_rate * (step_dir + decay_rate * master)
    return (new_master, new_first, new_second)


CHUNKS = 8
MESH = pl.DeviceIdType.MESH


def step_kernel(
    chunks,
    tokens,
    grad_t,
    master,
    base_hbm,
    first,
    second,
    bounds,
    diff_bounds,
    signs,
    matrix_half,
    matrix,
    projected,
    out_master,
    out_first,
    out_second,
    base,
    coded,
    rec0,
    sum0,
    rec1,
    sum1,
    rec2,
    sum2,
    rec3,
    gath,
    turned,
    effective,
    total,
    base_sem,
    send_sem,
    recv_sem,
    zsend,
    zrecv,
):
    outer, inner = lax.axis_index("outer"), lax.axis_index("inner")
    inner_count = lax.axis_size("inner")
    xs = 2
    zs = inner_count // xs
    y, c = outer // 2, outer % 2
    z, x = inner // xs, inner % xs
    rows = master.shape[0]
    width = tokens.shape[1] // chunks
    block_len = matrix.shape[0]
    blocks = width // block_len
    row_blocks = grad_t.shape[0] // block_len
    z_step = block_len // (xs * rows)
    scale = 1.0 / math.sqrt(block_len)
    mine1 = x * (1 - c) + y * c
    mine2 = y * (1 - c) + x * c
    core_peer = (y * 2 + 1 - c, inner)
    x_peer = (outer, z * xs + 1 - x)
    y_peer = ((1 - y) * 2 + c, inner)
    peer1 = (x_peer[0] * (1 - c) + y_peer[0] * c, x_peer[1] * (1 - c) + y_peer[1] * c)
    peer2 = (y_peer[0] * (1 - c) + x_peer[0] * c, y_peer[1] * (1 - c) + x_peer[1] * c)
    z_ids = [lax.rem(z + k, zs) for k in range(1, zs)]
    z_peers = [(outer, zz * xs + x) for zz in z_ids]

    load_base = pltpu.make_async_copy(base_hbm, base, base_sem)
    load_base.start()
    barrier = pltpu.get_barrier_semaphore()
    peers = [core_peer, peer1, peer2] + z_peers
    for peer in peers:
        pl.semaphore_signal(barrier, inc=1, device_id=peer, device_id_type=MESH)
    total[...] = jnp.zeros_like(total)
    pl.semaphore_wait(barrier, len(peers))

    def remote(src, dst, stage, j, peer):
        return pltpu.make_async_remote_copy(
            src_ref=src,
            dst_ref=dst,
            send_sem=send_sem.at[stage, j],
            recv_sem=recv_sem.at[stage, j],
            device_id=peer,
            device_id_type=MESH,
        )

    def remote_z(src, dst, stage, j, k):
        return pltpu.make_async_remote_copy(
            src_ref=src,
            dst_ref=dst,
            send_sem=zsend.at[stage, j, k],
            recv_sem=zrecv.at[stage, j, k],
            device_id=z_peers[k],
            device_id_type=MESH,
        )

    def copy0(j):
        return remote(coded.at[j, 1 - c], rec0.at[j], 0, j, core_peer)

    def copy1(j):
        return remote(sum0.at[j, 1 - mine1], rec1.at[j], 1, j, peer1)

    def copy2(j):
        return remote(sum1.at[j, 1 - mine2], rec2.at[j], 2, j, peer2)

    def copy3(j):
        return [remote_z(sum2.at[j, z_ids[k]], rec3.at[j, k], 0, j, k) for k in range(zs - 1)]

    def gather0(j):
        block = gath.at[j, c, mine1, mine2, z]
        return [remote_z(block, block, 1, j, k) for k in range(zs - 1)]

    def gather1(j):
        block = gath.at[j, c, mine1, mine2]
        return remote(block, block, 3, j, peer2)

    def gather2(j):
        block = gath.at[j, c, mine1]
        return remote(block, block, 4, j, peer1)

    def gather3(j):
        block = gath.at[j, c]
        return remote(block, block, 5, j, core_peer)

    def added(left, right):
        return (left.astype(jnp.float32) + right.astype(jnp.float32)).astype(jnp.bfloat16)

    def columns(j):
        return pl.ds(pl.multiple_of(j * width, width), width)

    def produce(j):
        for b in range(blocks):
            at = pl.ds(pl.multiple_of(j * width + b * block_len, block_len), block_len)
            part = jnp.dot(
                tokens[:, at] * signs[:, at].astype(jnp.bfloat16),
                matrix_half[...],
                preferred_element_type=jnp.float32,
            )
            turned[:, b * block_len : (b + 1) * block_len] = (part * scale).astype(jnp.bfloat16)

        def one(m, carry):
            part = jnp.dot(
                grad_t[pl.ds(pl.multiple_of(m * block_len, block_len), block_len), :],
                turned[...],
                preferred_element_type=jnp.float32,
            )
            limit = bounds[pl.ds(m, 1), columns(j)]
            part = jnp.minimum(jnp.maximum(part, -limit), limit).astype(jnp.bfloat16)
            per = row_blocks // 4
            group = m // per
            z0 = (m - group * per) * z_step
            coded[j, group % 2, group // 2, pl.ds(z0, z_step)] = part.reshape(
                z_step, xs, rows, width
            )
            return carry

        lax.fori_loop(0, row_blocks, one, 0)
        copy0(j).start()

    def reduce0(j):
        copy0(j).wait()
        for yy in range(2):
            for zz in range(zs):
                for xx in range(xs):
                    to1 = xx * (1 - c) + yy * c
                    to2 = yy * (1 - c) + xx * c
                    sum0[j, to1, to2, zz] = added(coded[j, c, yy, zz, xx], rec0[j, yy, zz, xx])
        copy1(j).start()

    def reduce1(j):
        copy1(j).wait()
        sum1[j] = added(sum0[j, mine1], rec1[j])
        copy2(j).start()

    def reduce2(j):
        copy2(j).wait()
        sum2[j] = added(sum1[j, mine2], rec2[j])
        for item in copy3(j):
            item.start()

    def update(j):
        copies = copy3(j)
        for item in copies:
            item.wait()
        summed = sum2[j, z].astype(jnp.float32)
        for k in range(zs - 1):
            summed = summed + rec3[j, k].astype(jnp.float32)
        own = pl.ds(pl.multiple_of((outer * inner_count + inner) * rows, rows), rows)
        for b in range(blocks):
            at = pl.ds(pl.multiple_of(j * width + b * block_len, block_len), block_len)
            gradient = (
                jnp.dot(
                    summed[:, b * block_len : (b + 1) * block_len],
                    matrix[...],
                    precision=highest,
                    preferred_element_type=jnp.float32,
                )
                * scale
                * signs[:, at]
            )
            new_master, new_first, new_second = adam_update(
                gradient, master[:, at], first[:, at], second[:, at]
            )
            out_master[:, at] = new_master
            out_first[:, at] = new_first
            out_second[:, at] = new_second
            limit = diff_bounds[j, :, b : b + 1]
            change = new_master - base[own, at].astype(jnp.float32)
            change = jnp.minimum(jnp.maximum(change, -limit), limit)
            gath[j, c, mine1, mine2, z, :, b * block_len : (b + 1) * block_len] = change.astype(
                jnp.bfloat16
            )
        for item in gather0(j):
            item.start()

    def pass1(j):
        for item in gather0(j):
            item.wait()
        gather1(j).start()

    def pass2(j):
        gather1(j).wait()
        gather2(j).start()

    def pass3(j):
        gather2(j).wait()
        gather3(j).start()

    def consume(j):
        gather3(j).wait()
        for yy in range(2):
            for cc in range(2):
                group = yy * 2 + cc
                count = zs * xs * rows
                for zz in range(zs):
                    for xx in range(xs):
                        at1, at2 = (xx, yy) if cc == 0 else (yy, xx)
                        low = (zz * xs + xx) * rows
                        effective[low : low + rows, :] = added(
                            base[group * count + low : group * count + low + rows, columns(j)],
                            gath[j, cc, at1, at2, zz],
                        )
                total[:, group * count : (group + 1) * count] += lax.dot_general(
                    tokens[:, columns(j)],
                    effective[...],
                    (((1,), (1,)), ((), ())),
                    preferred_element_type=jnp.float32,
                )

    stages = (produce, reduce0, reduce1, reduce2, update, pass1, pass2, pass3, consume)

    def step(t, carry):
        for place, stage in enumerate(stages):
            j = t - place

            @pl.when((j >= 0) & (j < chunks))
            def _():
                stage(j)

        return carry

    lax.fori_loop(0, 4, step, 0)
    load_base.wait()
    lax.fori_loop(4, chunks + len(stages) - 1, step, 0)
    projected[...] = total[...].astype(jnp.bfloat16)


def fused_step(tokens, out_grad, master, base, first, second, bounds, diff_bounds, signs, matrix):
    rows, model_width = master.shape
    features = out_grad.shape[1]
    inner_count = lax.axis_size("inner")
    zs = inner_count // 2
    width = model_width // CHUNKS
    vmem = pl.BlockSpec(memory_space=pltpu.VMEM)
    half = jnp.bfloat16
    cell = (rows, width)
    flops = 4 * tokens.shape[0] * model_width * features
    return pl.pallas_call(
        functools.partial(step_kernel, CHUNKS),
        out_shape=(
            jax.ShapeDtypeStruct((tokens.shape[0], features), half),
            jax.ShapeDtypeStruct(master.shape, jnp.float32),
            jax.ShapeDtypeStruct(master.shape, jnp.float32),
            jax.ShapeDtypeStruct(master.shape, jnp.float32),
        ),
        in_specs=[vmem] * 3 + [pl.BlockSpec(memory_space=pl.ANY)] + [vmem] * 7,
        out_specs=(vmem,) * 4,
        scratch_shapes=[
            pltpu.VMEM(base.shape, half),
            pltpu.VMEM((CHUNKS, 2, 2, zs, 2) + cell, half),
            pltpu.VMEM((CHUNKS, 2, zs, 2) + cell, half),
            pltpu.VMEM((CHUNKS, 2, 2, zs) + cell, half),
            pltpu.VMEM((CHUNKS, 2, zs) + cell, half),
            pltpu.VMEM((CHUNKS, 2, zs) + cell, half),
            pltpu.VMEM((CHUNKS, zs) + cell, half),
            pltpu.VMEM((CHUNKS, zs) + cell, half),
            pltpu.VMEM((CHUNKS, zs - 1) + cell, half),
            pltpu.VMEM((CHUNKS, 2, 2, 2, zs) + cell, half),
            pltpu.VMEM((tokens.shape[0], width), half),
            pltpu.VMEM((features // 4, width), half),
            pltpu.VMEM((tokens.shape[0], features), jnp.float32),
            pltpu.SemaphoreType.DMA,
            pltpu.SemaphoreType.DMA((6, CHUNKS)),
            pltpu.SemaphoreType.DMA((6, CHUNKS)),
            pltpu.SemaphoreType.DMA((2, CHUNKS, zs - 1)),
            pltpu.SemaphoreType.DMA((2, CHUNKS, zs - 1)),
        ],
        compiler_params=pltpu.CompilerParams(
            collective_id=0, has_side_effects=True, vmem_limit_bytes=66000000
        ),
        cost_estimate=pl.CostEstimate(flops=flops, bytes_accessed=2**25, transcendentals=0),
    )(
        tokens,
        out_grad.T,
        master,
        base,
        first,
        second,
        bounds,
        diff_bounds,
        signs,
        matrix.astype(half),
        matrix,
    )


def fits_kernel(token_rows, rows_dev, block_len, features, model_width):
    inner_count = lax.axis_size("inner")
    pair = 2 * rows_dev
    return (
        lax.axis_size("outer") == 4
        and inner_count % 2 == 0
        and inner_count > 2
        and rows_dev % 16 == 0
        and token_rows % 16 == 0
        and block_len % pair == 0
        and (inner_count * rows_dev) % block_len == 0
        and features == 4 * inner_count * rows_dev
        and model_width % (CHUNKS * block_len) == 0
        and features * model_width <= 2**22
    )


def shards(
    tokens,
    out_grad,
    master_weights,
    base_weights,
    adam_m,
    adam_v,
    grad_exps,
    diff_exps,
    hadamard_signs,
):
    outer_count = lax.axis_size("outer")
    inner_count = lax.axis_size("inner")
    token_rows = tokens.shape[0]
    model_width = tokens.shape[1]
    rows_dev = master_weights.shape[0]
    sign_rows = (2 * hadamard_signs - 1).astype(jnp.float32)
    block_len = sign_rows.shape[1]
    col_blocks = sign_rows.shape[0]
    matrix = hadamard(block_len)
    bound_all = jnp.repeat(
        clip_level * jnp.exp2(grad_exps[0].astype(jnp.float32)), block_len, axis=0
    )
    if fits_kernel(token_rows, rows_dev, block_len, out_grad.shape[1], model_width):
        limits = clip_level * jnp.exp2(grad_exps[0].astype(jnp.float32))
        diff_limits = clip_level * jnp.exp2(diff_exps.astype(jnp.float32))
        return fused_step(
            tokens,
            out_grad,
            master_weights,
            base_weights,
            adam_m,
            adam_v,
            jnp.repeat(limits, block_len, axis=1),
            diff_limits.reshape(rows_dev, CHUNKS, -1).transpose(1, 0, 2),
            sign_rows.reshape(1, -1),
            matrix,
        )
    grad_grid = out_grad.reshape(token_rows, outer_count, inner_count, rows_dev).transpose(
        0, 2, 1, 3
    )
    bound_grid = bound_all.reshape(outer_count, inner_count, rows_dev, col_blocks).transpose(
        1, 0, 2, 3
    )
    coded_bound_sel = bound_grid.reshape(-1, col_blocks)
    term_rows = lax.dot_general(
        grad_grid.reshape(token_rows, -1),
        tokens,
        (((0,), (0,)), ((), ())),
        preferred_element_type=jnp.float32,
    )
    turned = rotate_rows(term_rows, sign_rows, matrix)
    coded_rows = lax.optimization_barrier(clip_rows(turned, coded_bound_sel).astype(jnp.bfloat16))
    coded_rows = coded_rows.astype(jnp.float32)
    group_sum = lax.psum_scatter(
        coded_rows.reshape(1 * lax.axis_size("inner"), outer_count, rows_dev, model_width).astype(
            jnp.bfloat16
        ),
        "inner",
        scatter_dimension=0,
        tiled=True,
    )
    summed = (
        lax.psum_scatter(group_sum, "outer", scatter_dimension=1, tiled=True)
        .astype(jnp.float32)
        .reshape(rows_dev, model_width)
    )
    gradient = unrotate_rows(summed, sign_rows, matrix)
    new_master, new_first, new_second = adam_update(gradient, master_weights, adam_m, adam_v)
    owner = lax.axis_index("outer") * inner_count + lax.axis_index("inner")
    base_own = lax.dynamic_slice_in_dim(base_weights, owner * rows_dev, rows_dev, 0).astype(
        jnp.float32
    )
    diff_bound = clip_level * jnp.exp2(diff_exps.astype(jnp.float32))
    diff_coded = clip_rows(new_master - base_own, diff_bound).astype(jnp.bfloat16)
    effective = (
        base_weights.astype(jnp.float32)
        + lax.all_gather(diff_coded, ("outer", "inner"), axis=0, tiled=True).astype(jnp.float32)
    ).astype(jnp.bfloat16)
    result = lax.dot_general(
        tokens, effective, (((1,), (1,)), ((), ())), preferred_element_type=jnp.float32
    )
    projected = result.astype(jnp.bfloat16)
    return (projected, new_master, new_first, new_second)


def solution(mesh):
    in_specs = (
        P(("outer", "inner"), None),
        P(("outer", "inner"), None),
        P(("outer", "inner"), None),
        P(),
        P(("outer", "inner"), None),
        P(("outer", "inner"), None),
        P(("outer", "inner"), None, None),
        P(("outer", "inner"), None),
        P(),
    )
    out_specs = (
        P(("outer", "inner"), None),
        P(("outer", "inner"), None),
        P(("outer", "inner"), None),
        P(("outer", "inner"), None),
    )
    return jax.shard_map(shards, mesh=mesh, in_specs=in_specs, out_specs=out_specs, check_vma=False)
```
